32 devices in a mesh: dev: 8 (over z, x), rep: 4 (over y, core).
Axes of the slice: x: 2, y: 2, z: 4, core: 2. Of those that a mesh axis runs over, the one named last changes fastest.
Arguments:
- emb_table: float32 [32768, 160], P('dev'), may hold values from -6 to 6
- feature_ids: int32 [4096, 4, 8], P(('dev', 'rep')), may hold values from 0 to 8191
- lengths: int32 [4096, 4], P(('dev', 'rep')), may hold values from 1 to 8
- cotangent: float32 [4096, 4, 160], P(('dev', 'rep')), may hold values from -6 to 6
Outputs:
- pooled: float32 [4096, 4, 160], P(('dev', 'rep'))
- row_grads: float32 [32768, 160], P(('dev', 'rep'))
The draws below stay inside these ranges and needn't reach their ends.
All inputs are finite; a program needn't handle non-finite values.
Results may differ from the reference program's by a relative error of at most 0.00008.
Values sent between devices are 32-bit elements; how exact they have to be, the bound alone decides.
A program may use at most 128 MiB of HBM per device.

```python
import math
import jax
import jax.numpy as jnp
import numpy as np
from jax import lax

E = 160
FEATS = 4
BAG = 8
ROWS_DEV = 4096
ROWS = 32768
VOCAB = 8192
BATCH = 4096
N_DEV = 8


def touch_ends(entries, rng, low, largest):
    place = [jax.random.randint(jax.random.fold_in(rng, axis), (), 0, length) for axis, length in enumerate(entries.shape)]
    longest = entries.shape.index(max(entries.shape))
    beside = place[:longest] + [(place[longest] + 1) % entries.shape[longest]] + place[longest + 1:]
    return entries.at[tuple(place)].set(low).at[tuple(beside)].set(largest)


def steps_of(key, dims, pieces, smallest, high):
    loudness, own = 1.0, jax.random.fold_in(key, 6)
    for axis_at, blocks in pieces:
        draws = jnp.exp(jax.random.uniform(jax.random.fold_in(own, axis_at), (blocks,), jnp.float32, smallest / len(pieces), high / len(pieces)))
        loudness = loudness * jnp.repeat(draws, dims[axis_at] // blocks).reshape([-1 if axis == axis_at else 1 for axis in range(len(dims))])
    return loudness


def rank_table(amount, skew):
    loads = [(1 << 20) // math.isqrt(rank ** skew) + 1 for rank in range(1, amount + 1)]
    deviation = 1 + sum(loads) // (1 << 30)
    return np.cumsum(np.array([max(1, weight // deviation) for weight in loads]))


def ranked(stream_key, shape, count, lean):
    grid = rank_table(count, lean)
    ticket = jax.random.randint(jax.random.fold_in(stream_key, 1), shape, 0, int(grid[count - 1]))
    grade = jnp.searchsorted(jnp.asarray(grid, jnp.int32), ticket, side="right")
    return jax.random.permutation(jax.random.fold_in(stream_key, 2), count)[grade].astype(jnp.int32)


def centred(key, dims, deviation, limit, split=(), held_as=jnp.bfloat16):
    drawn = deviation * jax.random.normal(key, dims, jnp.float32)
    if split:
        drawn = drawn * steps_of(key, dims, split, -0.22, 0.18)
    return jnp.clip(drawn, -limit, limit).astype(held_as)


def setup_inputs(seed: int = 0) -> dict:
    key_list = jax.random.split(jax.random.key(seed), 5)
    return {
        "emb_table": centred(key_list[0], (ROWS, E), 1.0, 6.0, ((0, 8),), jnp.float32),
        "feature_ids": touch_ends(ranked(key_list[1], (BATCH, FEATS, BAG), VOCAB, 2), jax.random.fold_in(key_list[1], 3), 0, VOCAB - 1).astype(jnp.int32),
        "lengths": touch_ends(jax.random.randint(key_list[2], (BATCH, FEATS), 1, BAG + 1), jax.random.fold_in(key_list[2], 1), 1, BAG).astype(jnp.int32),
        "cotangent": centred(key_list[3], (BATCH, FEATS, E), 1.0, 6.0, ((0, 32),), jnp.float32),
    }


def reference(emb_table, feature_ids, lengths, cotangent):
    vocabulary = ROWS_DEV * N_DEV // FEATS
    slot_index = jnp.arange(BAG, dtype=jnp.int32)
    live_slots = slot_index[None, None, :] < lengths[:, :, None]
    share = 1.0 / lengths.astype(jnp.float32)
    weights = jnp.where(live_slots, share[:, :, None], 0.0).astype(jnp.float32)
    offsets = (jnp.arange(FEATS, dtype=jnp.int32) * vocabulary).astype(jnp.int32)
    global_ids = (feature_ids + offsets[None, :, None]).astype(jnp.int32)

    def pool_feature(inputs):
        feature_rows, feature_weights = inputs
        gathered = emb_table[feature_rows]
        return jnp.sum(gathered * feature_weights[:, :, None], axis=1)

    pooled = lax.map(pool_feature, (jnp.transpose(global_ids, (1, 0, 2)), jnp.transpose(weights, (1, 0, 2))))
    pooled = jnp.transpose(pooled, (1, 0, 2))

    def add_feature(running, inputs):
        feature_rows, feature_weights, feature_cot = inputs
        contrib = feature_weights[:, :, None] * feature_cot[:, None, :]
        running = running.at[feature_rows.reshape(-1)].add(contrib.reshape(-1, E))
        return running, None

    start_grads = jnp.zeros((ROWS_DEV * N_DEV, E), jnp.float32)
    row_grads, _ = lax.scan(add_feature, start_grads, (jnp.transpose(global_ids, (1, 0, 2)), jnp.transpose(weights, (1, 0, 2)), jnp.transpose(cotangent, (1, 0, 2))))
    return pooled, row_grads
```

```python
import functools

import jax
import jax.numpy as jnp
from jax import lax
from jax.experimental import pallas as pl
from jax.experimental.pallas import tpu as pltpu
from jax.sharding import PartitionSpec as P

F32, BF16, I32 = jnp.float32, jnp.bfloat16, jnp.int32
ROW_TILE = 256


def split_bits(value):
    high = value.astype(BF16)
    low = (value - high.astype(F32)).astype(BF16)
    return high, low


def kernel(
    n, reps, table, ids, lens, cot, pooled, grads,
    ids_buf, cot_buf, counts, halves, part, part_in, scaled, total, landed,
    id_send, id_recv, cot_send, cot_recv, part_send, part_recv, row_send, row_recv,
):
    features, bag, each = ids.shape
    width, rows_dev = table.shape
    owners = n // features
    rows_out = rows_dev // reps
    levels = reps.bit_length() - 1
    me = lax.axis_index("dev")
    rep = lax.axis_index("rep")
    feature = me // owners
    base = me % owners * rows_dev

    def flipped(value, bit):
        return value + (1 - 2 * (value // (1 << bit) % 2)) * (1 << bit)

    barrier = pltpu.get_barrier_semaphore()
    for step in range(1, n):
        pl.semaphore_signal(
            barrier, inc=1, device_id={"dev": (me + step) % n},
            device_id_type=pl.DeviceIdType.MESH,
        )
    for level in range(levels):
        pl.semaphore_signal(
            barrier, inc=1, device_id={"rep": flipped(rep, level)},
            device_id_type=pl.DeviceIdType.MESH,
        )
    pl.semaphore_wait(barrier, n - 1 + levels)

    def id_copy(peer, source):
        return pltpu.make_async_remote_copy(
            src_ref=ids.at[peer // owners], dst_ref=ids_buf.at[source],
            send_sem=id_send.at[peer], recv_sem=id_recv.at[source],
            device_id={"dev": peer}, device_id_type=pl.DeviceIdType.MESH,
        )

    def cot_copy(peer, source):
        return pltpu.make_async_remote_copy(
            src_ref=cot.at[peer // owners], dst_ref=cot_buf.at[source],
            send_sem=cot_send.at[peer], recv_sem=cot_recv.at[source],
            device_id={"dev": peer}, device_id_type=pl.DeviceIdType.MESH,
        )

    def part_copy(peer, source):
        return pltpu.make_async_remote_copy(
            src_ref=part.at[peer], dst_ref=part_in.at[source],
            send_sem=part_send.at[peer], recv_sem=part_recv.at[source],
            device_id={"dev": peer}, device_id_type=pl.DeviceIdType.MESH,
        )

    for step in range(1, n):
        id_copy((me + step) % n, me).start()
    for step in range(1, n):
        cot_copy((me + step) % n, me).start()

    ids_buf[me] = ids[feature]
    cot_buf[me] = cot[feature]

    def split_table(tile, _):
        at = pl.ds(pl.multiple_of(tile * ROW_TILE, ROW_TILE), ROW_TILE)
        high, low = split_bits(table[:, at])
        halves[:width, at] = high
        halves[width:, at] = low
        return 0

    lax.fori_loop(0, rows_dev // ROW_TILE, split_table, 0)

    def pool_pair(pair, _):
        columns = pl.ds(pl.multiple_of(pair * 2 * each, 2 * each), 2 * each)
        blocks = []
        for half in range(2):
            step = pair * 2 + half
            source = (me - step + n) % n

            @pl.when(step > 0)
            def _():
                id_copy(source, source).wait_recv()

            blocks.append(ids_buf[source])
        slots = jnp.concatenate(blocks, axis=1) - base
        keys, times = [], []
        for j in range(bag):
            own = slots[j : j + 1]
            same = (slots == own).astype(I32)
            repeat = jnp.sum(same, axis=0, keepdims=True)
            keep = (own >= 0) & (own < rows_dev)
            if j:
                keep = keep & (jnp.sum(same[:j], axis=0, keepdims=True) == 0)
            keys.append(jnp.where(keep, own, -1))
            times.append(jnp.broadcast_to(repeat.astype(F32), (16, 2 * each)).astype(BF16))

        def count_tile(tile, _):
            start = pl.multiple_of(tile * ROW_TILE, ROW_TILE)
            wanted = []
            for j in range(bag):
                local = keys[j] - start
                local = jnp.where((local >= 0) & (local < ROW_TILE), local, -1)
                wanted.append(jnp.broadcast_to(local.astype(F32), (16, 2 * each)).astype(BF16))
            row = lax.broadcasted_iota(I32, (16, 2 * each), 0).astype(F32)
            for group in range(ROW_TILE // 16):
                here = (row + 16.0 * group).astype(BF16)
                found = jnp.zeros((16, 2 * each), BF16)
                for j in range(bag):
                    found = jnp.where(wanted[j] == here, times[j], found)
                counts[pl.ds(start + 16 * group, 16), columns] = found
            return 0

        lax.fori_loop(0, rows_dev // ROW_TILE, count_tile, 0)
        both = jnp.dot(halves[...], counts[:, columns], preferred_element_type=F32)
        pool = both[:width] + both[width:]
        for half in range(2):
            step = pair * 2 + half
            source = (me - step + n) % n
            mine = pool[:, half * each : (half + 1) * each]

            @pl.when(step == 0)
            def _():
                part_in[me] = mine

            @pl.when(step > 0)
            def _():
                part[source] = mine
                part_copy(source, me).start()

        return 0

    lax.fori_loop(0, n // 2, pool_pair, 0)

    def scale_step(step, _):
        source = (me - step + n) % n

        @pl.when(step > 0)
        def _():
            cot_copy(source, source).wait_recv()

        live = jnp.sum((ids_buf[source] >= 0).astype(F32), axis=0, keepdims=True)
        high, low = split_bits(cot_buf[source] * (1.0 / live))
        columns = pl.ds(pl.multiple_of(step * each, each), each)
        scaled[:width, columns] = high
        scaled[width:, columns] = low
        return 0

    lax.fori_loop(0, n, scale_step, 0)

    def grad_chunk(chunk, level, target):
        def grad_tile(tile, _):
            start = pl.multiple_of(tile * ROW_TILE, ROW_TILE)
            rows = pl.ds(pl.multiple_of(chunk * rows_out + start, ROW_TILE), ROW_TILE)
            both = lax.dot_general(
                scaled[...], counts[rows, :], (((1,), (1,)), ((), ())),
                preferred_element_type=F32,
            )
            target[:, pl.ds(start, ROW_TILE)] = both[:width] + both[width:]
            return 0

        lax.fori_loop(0, rows_out // ROW_TILE, grad_tile, 0)

    sent, first = [], [0]
    for level in range(levels):
        first.append(first[-1] + (1 << (levels - 1 - level)))

    def gather_in(chunk, level, target):
        for before in range(level):
            target[...] = target[...] + landed[first[before] + chunk // (1 << (before + 1))]

    def row_copy(slot, level):
        return pltpu.make_async_remote_copy(
            src_ref=total.at[slot], dst_ref=landed.at[slot],
            send_sem=row_send.at[slot], recv_sem=row_recv.at[slot],
            device_id={"rep": flipped(rep, level)}, device_id_type=pl.DeviceIdType.MESH,
        )

    def wait_level(level):
        for slot in range(first[level], first[level + 1]):
            row_copy(slot, level).wait_recv()

    for level in range(levels):
        span = 1 << (levels - 1 - level)
        chunks = []
        for far in reversed(range(span)):
            high = rep // (1 << (level + 1))
            for bit in range(levels):
                if far >> bit & 1:
                    high = flipped(high, bit)
            low = rep % (1 << level)
            other = 1 - rep // (1 << level) % 2
            chunk = (high * 2 + other) * (1 << level) + low
            chunks.append((first[level] + high, chunk))
        for slot, chunk in chunks:
            grad_chunk(chunk, level, total.at[slot])
            if level == 0:
                row_copy(slot, level).start()
        if level:
            wait_level(level - 1)
            for slot, chunk in chunks:
                gather_in(chunk, level, total.at[slot])
                row_copy(slot, level).start()
        sent.extend((slot, level) for slot, _ in chunks)
    grad_chunk(rep, levels, grads)

    for step in range(1, n):
        part_copy((me - step + n) % n, (me - step + n) % n).wait_recv()
    for feature_at in range(features):
        value = part_in[feature_at * owners]
        for owner in range(1, owners):
            value = value + part_in[feature_at * owners + owner]
        pooled[feature_at] = value * (1.0 / lens[feature_at : feature_at + 1].astype(F32))

    wait_level(levels - 1)
    gather_in(rep, levels, grads)
    for slot, level in sent:
        row_copy(slot, level).wait_send()
    for step in range(1, n):
        peer = (me + step) % n
        id_copy(peer, me).wait_send()
        cot_copy(peer, me).wait_send()
        part_copy(peer, me).wait_send()


def body(n, reps, emb_table, feature_ids, lengths, cotangent):
    rows_dev, width = emb_table.shape
    each, features, bag = feature_ids.shape
    ids = jnp.transpose(feature_ids, (1, 2, 0))
    lens = lengths.T
    slot_index = lax.broadcasted_iota(I32, ids.shape, 1)
    ids = jnp.where(slot_index < lens[:, None, :], ids, -(1 << 20))
    rows_out = rows_dev // reps
    sem = pltpu.SemaphoreType.DMA
    pooled, grads = pl.pallas_call(
        functools.partial(kernel, n, reps),
        out_shape=(
            jax.ShapeDtypeStruct((features, width, each), F32),
            jax.ShapeDtypeStruct((width, rows_out), F32),
        ),
        in_specs=[pl.BlockSpec(memory_space=pltpu.VMEM)] * 4,
        out_specs=[pl.BlockSpec(memory_space=pltpu.VMEM)] * 2,
        scratch_shapes=[
            pltpu.VMEM((n, bag, each), I32),
            pltpu.VMEM((n, width, each), F32),
            pltpu.VMEM((rows_dev, n * each), BF16),
            pltpu.VMEM((2 * width, rows_dev), BF16),
            pltpu.VMEM((n, width, each), F32),
            pltpu.VMEM((n, width, each), F32),
            pltpu.VMEM((2 * width, n * each), BF16),
            pltpu.VMEM((reps - 1, width, rows_out), F32),
            pltpu.VMEM((reps - 1, width, rows_out), F32),
            sem((n,)), sem((n,)), sem((n,)), sem((n,)), sem((n,)), sem((n,)),
            sem((reps - 1,)), sem((reps - 1,)),
        ],
        compiler_params=pltpu.CompilerParams(
            collective_id=0, has_side_effects=True, vmem_limit_bytes=60 * 1024 * 1024
        ),
    )(emb_table.T, ids, lens, jnp.transpose(cotangent, (1, 2, 0)))
    return jnp.transpose(pooled, (2, 0, 1)), grads.T


def solution(mesh):
    return jax.shard_map(
        functools.partial(body, mesh.shape["dev"], mesh.shape["rep"]),
        mesh=mesh,
        in_specs=(
            P("dev", None),
            P(("dev", "rep"), None, None),
            P(("dev", "rep"), None),
            P(("dev", "rep"), None, None),
        ),
        out_specs=(P(("dev", "rep"), None, None), P(("dev", "rep"), None)),
        check_vma=False,
    )
```

```python
import functools

import jax
import jax.numpy as jnp
from jax import lax
from jax.experimental import pallas as pl
from jax.experimental.pallas import tpu as pltpu
from jax.sharding import PartitionSpec as P

F32, BF16, I32 = jnp.float32, jnp.bfloat16, jnp.int32
ROW_TILE = 256


def split_bits(value):
    high = value.astype(BF16)
    low = (value - high.astype(F32)).astype(BF16)
    return high, low


def kernel(
    n, reps, table, ids, lens, cot, pooled, grads,
    ids_buf, cot_buf, counts, halves, part, part_in, pool_in, scaled, total, landed,
    id_send, id_recv, cot_send, cot_recv, pass_send,
    part_send, part_recv, pool_send, pool_recv, row_send, row_recv,
):
    features, bag, each = ids.shape
    width, rows_dev = table.shape
    owners = n // features
    rows_out = rows_dev // reps
    levels = reps.bit_length() - 1
    pairs = n // 2
    me = lax.axis_index("dev")
    rep = lax.axis_index("rep")
    feature = me // owners
    lane = me % owners
    base = lane * rows_dev

    def flipped(value, bit):
        return value + (1 - 2 * (value // (1 << bit) % 2)) * (1 << bit)

    def near(step):
        return (me + step) % n

    def beside(step):
        return feature * owners + (lane + step) % owners

    def across(step):
        return (feature + step) % features * owners + lane

    barrier = pltpu.get_barrier_semaphore()
    for step in range(1, n):
        pl.semaphore_signal(
            barrier, inc=1, device_id={"dev": near(step)}, device_id_type=pl.DeviceIdType.MESH
        )
    for level in range(levels):
        pl.semaphore_signal(
            barrier, inc=1, device_id={"rep": flipped(rep, level)},
            device_id_type=pl.DeviceIdType.MESH,
        )
    pl.semaphore_wait(barrier, n - 1 + levels)

    def remote(src, dst, send, recv, axis, to):
        return pltpu.make_async_remote_copy(
            src_ref=src, dst_ref=dst, send_sem=send, recv_sem=recv,
            device_id={axis: to}, device_id_type=pl.DeviceIdType.MESH,
        )

    def id_copy(peer, source):
        return remote(
            ids.at[peer // owners], ids_buf.at[source],
            id_send.at[peer], id_recv.at[source], "dev", peer,
        )

    def cot_copy(peer, source):
        return remote(
            cot.at[peer // owners], cot_buf.at[source],
            cot_send.at[peer], cot_recv.at[source], "dev", peer,
        )

    def pass_copy(source, step):
        return remote(
            cot_buf.at[source], cot_buf.at[source],
            pass_send.at[source // owners, step], cot_recv.at[source], "dev", beside(step),
        )

    def part_copy(source, slot):
        return remote(
            part.at[source], part_in.at[slot], part_send.at[source], part_recv.at[slot],
            "dev", feature * owners + source % owners,
        )

    def pool_copy(source, slot):
        return remote(
            part.at[source], pool_in.at[slot],
            pool_send.at[source // owners], pool_recv.at[slot], "dev", source,
        )

    for step in range(1, n):
        id_copy(near(step), me).start()
    for step in range(1, owners):
        cot_copy(beside(step), me).start()
    for step in range(1, features):
        cot_copy(across(step), me).start()

    ids_buf[me] = ids[feature]
    cot_buf[me] = cot[feature]

    def split_table(tile, _):
        at = pl.ds(pl.multiple_of(tile * ROW_TILE, ROW_TILE), ROW_TILE)
        high, low = split_bits(table[:, at])
        halves[:width, at] = high
        halves[width:, at] = low
        return 0

    lax.fori_loop(0, rows_dev // ROW_TILE, split_table, 0)

    def pass_on(step):
        source = across(features - step)
        cot_copy(source, source).wait_recv()
        for side in range(1, owners):
            pass_copy(source, side).start()

    def pair_columns(pair):
        return pl.ds(pl.multiple_of(pair * 2 * each, 2 * each), 2 * each)

    def count_pair(pair, _):
        columns = pair_columns(pair)
        blocks = []
        for half in range(2):
            step = pair * 2 + half
            source = (me - step + n) % n

            @pl.when(step > 0)
            def _():
                id_copy(source, source).wait_recv()

            blocks.append(ids_buf[source])
        slots = jnp.concatenate(blocks, axis=1) - base
        keys, times = [], []
        for j in range(bag):
            own = slots[j : j + 1]
            same = (slots == own).astype(I32)
            repeat = jnp.sum(same, axis=0, keepdims=True)
            keep = (own >= 0) & (own < rows_dev)
            if j:
                keep = keep & (jnp.sum(same[:j], axis=0, keepdims=True) == 0)
            keys.append(jnp.where(keep, own, -1))
            times.append(jnp.broadcast_to(repeat.astype(F32), (16, 2 * each)).astype(BF16))

        def count_tile(tile, _):
            start = pl.multiple_of(tile * ROW_TILE, ROW_TILE)
            wanted = []
            for j in range(bag):
                local = keys[j] - start
                local = jnp.where((local >= 0) & (local < ROW_TILE), local, -1)
                wanted.append(jnp.broadcast_to(local.astype(F32), (16, 2 * each)).astype(BF16))
            row = lax.broadcasted_iota(I32, (16, 2 * each), 0).astype(F32)
            for group in range(ROW_TILE // 16):
                here = (row + 16.0 * group).astype(BF16)
                found = jnp.zeros((16, 2 * each), BF16)
                for j in range(bag):
                    found = jnp.where(wanted[j] == here, times[j], found)
                counts[pl.ds(start + 16 * group, 16), columns] = found
            return 0

        lax.fori_loop(0, rows_dev // ROW_TILE, count_tile, 0)

        @pl.when((pair > 0) & (pair < features))
        def _():
            pass_on(pair)

        return 0

    lax.fori_loop(0, pairs, count_pair, 0)
    for step in range(pairs, features):
        pass_on(step)

    def scale_step(step, _):
        source = (me - step + n) % n

        @pl.when(source % owners != lane)
        def _():
            cot_copy(source, source).wait_recv()

        live = jnp.sum((ids_buf[source] >= 0).astype(F32), axis=0, keepdims=True)
        high, low = split_bits(cot_buf[source] * (1.0 / live))
        columns = pl.ds(pl.multiple_of(step * each, each), each)
        scaled[:width, columns] = high
        scaled[width:, columns] = low
        return 0

    lax.fori_loop(0, n, scale_step, 0)

    def grad_chunk(chunk, target):
        def grad_tile(tile, _):
            start = pl.multiple_of(tile * ROW_TILE, ROW_TILE)
            rows = pl.ds(pl.multiple_of(chunk * rows_out + start, ROW_TILE), ROW_TILE)
            both = lax.dot_general(
                scaled[...], counts[rows, :], (((1,), (1,)), ((), ())),
                preferred_element_type=F32,
            )
            target[:, pl.ds(start, ROW_TILE)] = both[:width] + both[width:]
            return 0

        lax.fori_loop(0, rows_out // ROW_TILE, grad_tile, 0)

    first = [0]
    for level in range(levels):
        first.append(first[-1] + (1 << (levels - 1 - level)))

    def row_copy(slot, level):
        return remote(
            total.at[slot], landed.at[slot], row_send.at[slot], row_recv.at[slot],
            "rep", flipped(rep, level),
        )

    def pool_pair(pair, _):
        both = jnp.dot(halves[...], counts[:, pair_columns(pair)], preferred_element_type=F32)
        pool = both[:width] + both[width:]
        for half in range(2):
            source = (me - (pair * 2 + half) + n) % n
            part[source] = pool[:, half * each : (half + 1) * each]

            @pl.when(source % owners != lane)
            def _():
                part_copy(source, source // owners * owners + lane).start()

        return 0

    def sum_parts(step):
        source = across(step)
        value = part[source]
        for side in range(1, owners):
            slot = source // owners * owners + (lane + side) % owners
            part_copy(source, slot).wait_recv()
            value = value + part_in[slot]
        if step:
            part[source] = value
            pool_copy(source, feature).start()
        else:
            pool_in[feature] = value

    sent = []
    for apart in reversed(range(reps)):
        if apart == reps // 2 - 1:
            lax.fori_loop(0, pairs, pool_pair, 0)
            for step in reversed(range(features)):
                sum_parts(step)
        level, chunk = 0, rep
        while level < levels and not apart >> level & 1:
            level += 1
        for bit in range(levels):
            if apart >> bit & 1:
                chunk = flipped(chunk, bit)
        target = grads
        if apart:
            slot = first[level] + chunk // (1 << (level + 1))
            target = total.at[slot]
        grad_chunk(chunk, target)
        for before in range(level):
            arrived = first[before] + chunk // (1 << (before + 1))
            if apart == 0 and before == levels - 1:
                for step in range(1, features):
                    pool_copy(across(step), across(step) // owners).wait_recv()
                for at in range(features):
                    pooled[at] = pool_in[at] * (1.0 / lens[at : at + 1].astype(F32))
            row_copy(arrived, before).wait_recv()
            target[...] = target[...] + landed[arrived]
        if apart:
            row_copy(slot, level).start()
            sent.append((slot, level))

    for slot, level in sent:
        row_copy(slot, level).wait_send()
    for step in range(1, n):
        id_copy(near(step), me).wait_send()
    for step in range(1, owners):
        cot_copy(beside(step), me).wait_send()
    for step in range(1, features):
        source = across(step)
        cot_copy(source, me).wait_send()
        pool_copy(source, feature).wait_send()
        for side in range(1, owners):
            pass_copy(source, side).wait_send()
    for at in range(features):
        for side in range(1, owners):
            source = at * owners + (lane + side) % owners
            part_copy(source, at * owners + lane).wait_send()


def body(n, reps, emb_table, feature_ids, lengths, cotangent):
    rows_dev, width = emb_table.shape
    each, features, bag = feature_ids.shape
    ids = jnp.transpose(feature_ids, (1, 2, 0))
    lens = lengths.T
    slot_index = lax.broadcasted_iota(I32, ids.shape, 1)
    ids = jnp.where(slot_index < lens[:, None, :], ids, -(1 << 20))
    rows_out = rows_dev // reps
    sem = pltpu.SemaphoreType.DMA
    pooled, grads = pl.pallas_call(
        functools.partial(kernel, n, reps),
        out_shape=(
            jax.ShapeDtypeStruct((features, width, each), F32),
            jax.ShapeDtypeStruct((width, rows_out), F32),
        ),
        in_specs=[pl.BlockSpec(memory_space=pltpu.VMEM)] * 4,
        out_specs=[pl.BlockSpec(memory_space=pltpu.VMEM)] * 2,
        scratch_shapes=[
            pltpu.VMEM((n, bag, each), I32),
            pltpu.VMEM((n, width, each), F32),
            pltpu.VMEM((rows_dev, n * each), BF16),
            pltpu.VMEM((2 * width, rows_dev), BF16),
            pltpu.VMEM((n, width, each), F32),
            pltpu.VMEM((n, width, each), F32),
            pltpu.VMEM((features, width, each), F32),
            pltpu.VMEM((2 * width, n * each), BF16),
            pltpu.VMEM((reps - 1, width, rows_out), F32),
            pltpu.VMEM((reps - 1, width, rows_out), F32),
            sem((n,)), sem((n,)), sem((n,)), sem((n,)), sem((features, n // features)),
            sem((n,)), sem((n,)), sem((features,)), sem((features,)),
            sem((reps - 1,)), sem((reps - 1,)),
        ],
        compiler_params=pltpu.CompilerParams(
            collective_id=0, has_side_effects=True, vmem_limit_bytes=60 * 1024 * 1024
        ),
    )(emb_table.T, ids, lens, jnp.transpose(cotangent, (1, 2, 0)))
    return jnp.transpose(pooled, (2, 0, 1)), grads.T


def solution(mesh):
    return jax.shard_map(
        functools.partial(body, mesh.shape["dev"], mesh.shape["rep"]),
        mesh=mesh,
        in_specs=(
            P("dev", None),
            P(("dev", "rep"), None, None),
            P(("dev", "rep"), None),
            P(("dev", "rep"), None, None),
        ),
        out_specs=(P(("dev", "rep"), None, None), P(("dev", "rep"), None)),
        check_vma=False,
    )
```

```python
import functools

import jax
import jax.numpy as jnp
from jax import lax
from jax.experimental import pallas as pl
from jax.experimental.pallas import tpu as pltpu
from jax.sharding import PartitionSpec as P

F32, BF16, I32 = jnp.float32, jnp.bfloat16, jnp.int32
ROW_TILE = 256


def split_bits(value):
    high = value.astype(BF16)
    low = (value - high.astype(F32)).astype(BF16)
    return high, low


def kernel(
    n, reps, table_in, ids_in, lens_in, cot_in, pool_in, grads, arrived_rows,
    table, raw, lens, cot, ids, stage, ids_buf, cot_buf, counts, halves, part, part_in, scaled, total, landed,
    id_send, id_recv, cot_send, cot_recv, pass_send,
    part_send, part_recv, pool_send, pool_recv, row_send, row_recv,
):
    features, bag, each = ids.shape
    width, rows_dev = table.shape
    owners = n // features
    rows_out = rows_dev // reps
    levels = reps.bit_length() - 1
    pairs = n // 2
    me = lax.axis_index("dev")
    rep = lax.axis_index("rep")
    feature = me // owners
    lane = me % owners
    base = lane * rows_dev

    def flipped(value, bit):
        return value + (1 - 2 * (value // (1 << bit) % 2)) * (1 << bit)

    def near(step):
        return (me + step) % n

    def beside(step):
        return feature * owners + (lane + step) % owners

    def across(step):
        return (feature + step) % features * owners + lane

    barrier = pltpu.get_barrier_semaphore()
    for step in range(1, n):
        pl.semaphore_signal(
            barrier, inc=1, device_id={"dev": near(step)}, device_id_type=pl.DeviceIdType.MESH
        )
    for level in range(levels):
        pl.semaphore_signal(
            barrier, inc=1, device_id={"rep": flipped(rep, level)},
            device_id_type=pl.DeviceIdType.MESH,
        )
    staged = [
        pltpu.make_async_copy(src, dst, stage.at[at])
        for at, (src, dst) in enumerate(
            ((ids_in, raw), (lens_in, lens), (cot_in, cot), (table_in, table))
        )
    ]
    for copy in staged:
        copy.start()
    staged[0].wait()
    staged[1].wait()
    slot_index = lax.broadcasted_iota(I32, (bag, each), 0)
    for at in range(features):
        ids[at] = jnp.where(slot_index < lens[at : at + 1], raw[at], -(1 << 20))
    staged[2].wait()
    ids_buf[me] = ids[feature]
    cot_buf[me] = cot[feature]
    pl.semaphore_wait(barrier, n - 1 + levels)

    def remote(src, dst, send, recv, axis, to):
        return pltpu.make_async_remote_copy(
            src_ref=src, dst_ref=dst, send_sem=send, recv_sem=recv,
            device_id={axis: to}, device_id_type=pl.DeviceIdType.MESH,
        )

    def id_copy(peer, source):
        return remote(
            ids.at[peer // owners], ids_buf.at[source],
            id_send.at[peer], id_recv.at[source], "dev", peer,
        )

    def cot_copy(peer, source):
        return remote(
            cot.at[peer // owners], cot_buf.at[source],
            cot_send.at[peer], cot_recv.at[source], "dev", peer,
        )

    def pass_copy(source, step):
        return remote(
            cot_buf.at[source], cot_buf.at[source],
            pass_send.at[source // owners, step], cot_recv.at[source], "dev", beside(step),
        )

    def part_copy(source, slot):
        return remote(
            part.at[source], part_in.at[slot], part_send.at[source], part_recv.at[slot],
            "dev", feature * owners + source % owners,
        )

    def pool_copy(source, slot):
        return remote(
            part.at[source], pool_in.at[slot],
            pool_send.at[source // owners], pool_recv.at[slot], "dev", source,
        )

    for step in range(1, n):
        id_copy(near(step), me).start()
    for step in range(1, owners):
        cot_copy(beside(step), me).start()
    for step in range(1, features):
        cot_copy(across(step), me).start()

    staged[3].wait()

    def split_table(tile, _):
        at = pl.ds(pl.multiple_of(tile * ROW_TILE, ROW_TILE), ROW_TILE)
        high, low = split_bits(table[:, at])
        halves[:width, at] = high
        halves[width:, at] = low
        return 0

    lax.fori_loop(0, rows_dev // ROW_TILE, split_table, 0)

    def pass_on(step):
        source = across(features - step)
        cot_copy(source, source).wait_recv()
        for side in range(1, owners):
            pass_copy(source, side).start()

    def pair_columns(pair):
        return pl.ds(pl.multiple_of(pair * 2 * each, 2 * each), 2 * each)

    def count_pair(pair, _):
        columns = pair_columns(pair)
        blocks = []
        for half in range(2):
            step = pair * 2 + half
            source = (me - step + n) % n

            @pl.when(step > 0)
            def _():
                id_copy(source, source).wait_recv()

            blocks.append(ids_buf[source])
        slots = jnp.concatenate(blocks, axis=1) - base
        keys, times = [], []
        for j in range(bag):
            own = slots[j : j + 1]
            same = (slots == own).astype(I32)
            repeat = jnp.sum(same, axis=0, keepdims=True)
            keep = (own >= 0) & (own < rows_dev)
            if j:
                keep = keep & (jnp.sum(same[:j], axis=0, keepdims=True) == 0)
            keys.append(jnp.where(keep, own, -1))
            times.append(jnp.broadcast_to(repeat.astype(F32), (16, 2 * each)).astype(BF16))

        def count_tile(tile, _):
            start = pl.multiple_of(tile * ROW_TILE, ROW_TILE)
            wanted = []
            for j in range(bag):
                local = keys[j] - start
                local = jnp.where((local >= 0) & (local < ROW_TILE), local, -1)
                wanted.append(jnp.broadcast_to(local.astype(F32), (16, 2 * each)).astype(BF16))
            row = lax.broadcasted_iota(I32, (16, 2 * each), 0).astype(F32)
            for group in range(ROW_TILE // 16):
                here = (row + 16.0 * group).astype(BF16)
                found = jnp.zeros((16, 2 * each), BF16)
                for j in range(bag):
                    found = jnp.where(wanted[j] == here, times[j], found)
                counts[pl.ds(start + 16 * group, 16), columns] = found
            return 0

        lax.fori_loop(0, rows_dev // ROW_TILE, count_tile, 0)

        @pl.when((pair > 0) & (pair < features))
        def _():
            pass_on(pair)

        return 0

    lax.fori_loop(0, pairs, count_pair, 0)
    for step in range(pairs, features):
        pass_on(step)

    def scale_step(step, _):
        source = (me - step + n) % n

        @pl.when(source % owners != lane)
        def _():
            cot_copy(source, source).wait_recv()

        live = jnp.sum((ids_buf[source] >= 0).astype(F32), axis=0, keepdims=True)
        high, low = split_bits(cot_buf[source] * (1.0 / live))
        columns = pl.ds(pl.multiple_of(step * each, each), each)
        scaled[:width, columns] = high
        scaled[width:, columns] = low
        return 0

    lax.fori_loop(0, n, scale_step, 0)

    def grad_tile(chunk, tile):
        start = pl.multiple_of(chunk * rows_out + tile * ROW_TILE, ROW_TILE)
        both = lax.dot_general(
            scaled[...], counts[pl.ds(start, ROW_TILE), :], (((1,), (1,)), ((), ())),
            preferred_element_type=F32,
        )
        return both[:width] + both[width:]

    first = [0]
    for level in range(levels):
        first.append(first[-1] + (1 << (levels - 1 - level)))

    tiles = rows_out // ROW_TILE

    def row_copy(slot, level, tile):
        return remote(
            total.at[slot, tile], landed.at[slot, tile],
            row_send.at[slot, tile], row_recv.at[slot, tile],
            "rep", flipped(rep, level),
        )

    def pool_pair(pair, _):
        both = jnp.dot(halves[...], counts[:, pair_columns(pair)], preferred_element_type=F32)
        pool = both[:width] + both[width:]
        for half in range(2):
            source = (me - (pair * 2 + half) + n) % n
            part[source] = pool[:, half * each : (half + 1) * each]

            @pl.when(source % owners != lane)
            def _():
                part_copy(source, source // owners * owners + lane).start()

        return 0

    def sum_parts(step):
        source = across(step)
        value = part[source]
        for side in range(1, owners):
            slot = source // owners * owners + (lane + side) % owners
            part_copy(source, slot).wait_recv()
            value = value + part_in[slot]
        if step:
            part[source] = value
            pool_copy(source, feature).start()
        else:
            pool_in[feature] = value

    def place(apart):
        level, chunk = 0, rep
        while level < levels and not apart >> level & 1:
            level += 1
        for bit in range(levels):
            if apart >> bit & 1:
                chunk = flipped(chunk, bit)
        return level, chunk, first[level] + chunk // (1 << (level + 1)) if apart else 0

    def make_tile(apart, tile):
        level, chunk, slot = place(apart)
        value = grad_tile(chunk, tile)
        for before in range(level):
            if apart or before < levels - 1:
                came = first[before] + chunk // (1 << (before + 1))
                row_copy(came, before, tile).wait_recv()
                value = value + landed[came, tile]
        if apart:
            total[slot, tile] = value
            row_copy(slot, level, tile).start()
        else:
            grads[:, tile * ROW_TILE : (tile + 1) * ROW_TILE] = value

    far = reps // 2
    for tile in range(tiles + 1):
        for apart in reversed(range(far, reps)):
            late = 1 - apart % 2
            if 0 <= tile - late < tiles:
                make_tile(apart, tile - late)
    lax.fori_loop(0, pairs, pool_pair, 0)
    for apart in reversed(range(far)):
        for tile in range(tiles):
            make_tile(apart, tile)
    for step in reversed(range(features)):
        sum_parts(step)
    for step in range(1, features):
        pool_copy(across(step), across(step) // owners).wait_recv()
    came = first[levels - 1] + rep // (1 << levels)
    for tile in range(tiles):
        row_copy(came, levels - 1, tile).wait_recv()
        arrived_rows[:, tile * ROW_TILE : (tile + 1) * ROW_TILE] = landed[came, tile]

    for apart in range(1, reps):
        level, _, slot = place(apart)
        for tile in range(tiles):
            row_copy(slot, level, tile).wait_send()
    for step in range(1, n):
        id_copy(near(step), me).wait_send()
    for step in range(1, owners):
        cot_copy(beside(step), me).wait_send()
    for step in range(1, features):
        source = across(step)
        cot_copy(source, me).wait_send()
        pool_copy(source, feature).wait_send()
        for side in range(1, owners):
            pass_copy(source, side).wait_send()
    for at in range(features):
        for side in range(1, owners):
            source = at * owners + (lane + side) % owners
            part_copy(source, at * owners + lane).wait_send()


def finish(lens, pool, own, arrived, pooled, grads):
    for at in range(pool.shape[0]):
        pooled[at] = pool[at] * (1.0 / lens[at : at + 1].astype(F32))
    grads[...] = own[...] + arrived[...]


def body(n, reps, emb_table, feature_ids, lengths, cotangent):
    rows_dev, width = emb_table.shape
    each, features, bag = feature_ids.shape
    lens = lengths.T
    rows_out = rows_dev // reps
    tiles = rows_out // ROW_TILE
    sem = pltpu.SemaphoreType.DMA
    vmem = pl.BlockSpec(memory_space=pltpu.VMEM)
    pool_shape = jax.ShapeDtypeStruct((features, width, each), F32)
    rows_shape = jax.ShapeDtypeStruct((width, rows_out), F32)
    pool, own, arrived = pl.pallas_call(
        functools.partial(kernel, n, reps),
        out_shape=(pool_shape, rows_shape, rows_shape),
        in_specs=[pl.BlockSpec(memory_space=pl.ANY)] * 4,
        out_specs=[vmem] * 3,
        scratch_shapes=[
            pltpu.VMEM((width, rows_dev), F32),
            pltpu.VMEM((features, bag, each), I32),
            pltpu.VMEM((features, each), I32),
            pltpu.VMEM((features, width, each), F32),
            pltpu.VMEM((features, bag, each), I32),
            sem((4,)),
            pltpu.VMEM((n, bag, each), I32),
            pltpu.VMEM((n, width, each), F32),
            pltpu.VMEM((rows_dev, n * each), BF16),
            pltpu.VMEM((2 * width, rows_dev), BF16),
            pltpu.VMEM((n, width, each), F32),
            pltpu.VMEM((n, width, each), F32),
            pltpu.VMEM((2 * width, n * each), BF16),
            pltpu.VMEM((reps - 1, tiles, width, ROW_TILE), F32),
            pltpu.VMEM((reps - 1, tiles, width, ROW_TILE), F32),
            sem((n,)), sem((n,)), sem((n,)), sem((n,)), sem((features, n // features)),
            sem((n,)), sem((n,)), sem((features,)), sem((features,)),
            sem((reps - 1, tiles)), sem((reps - 1, tiles)),
        ],
        compiler_params=pltpu.CompilerParams(
            collective_id=0, has_side_effects=True, vmem_limit_bytes=60 * 1024 * 1024
        ),
    )(
        emb_table.T, jnp.transpose(feature_ids, (1, 2, 0)), lens,
        jnp.transpose(cotangent, (1, 2, 0)),
    )
    pooled, grads = pl.pallas_call(
        finish,
        out_shape=(pool_shape, rows_shape),
        in_specs=[vmem] * 4,
        out_specs=[vmem] * 2,
    )(lens, pool, own, arrived)
    return jnp.transpose(pooled, (2, 0, 1)), grads.T


def solution(mesh):
    return jax.shard_map(
        functools.partial(body, mesh.shape["dev"], mesh.shape["rep"]),
        mesh=mesh,
        in_specs=(
            P("dev", None),
            P(("dev", "rep"), None, None),
            P(("dev", "rep"), None),
            P(("dev", "rep"), None, None),
        ),
        out_specs=(P(("dev", "rep"), None, None), P(("dev", "rep"), None)),
        check_vma=False,
    )
```

```python
import functools

import jax
import jax.numpy as jnp
from jax import lax
from jax.experimental import pallas as pl
from jax.experimental.pallas import tpu as pltpu
from jax.sharding import PartitionSpec as P

F32, BF16, I32 = jnp.float32, jnp.bfloat16, jnp.int32
ROW_TILE = 256


def split_bits(value):
    high = value.astype(BF16)
    low = (value - high.astype(F32)).astype(BF16)
    return high, low


def kernel(
    n, reps, table_in, ids_in, lens_in, cot_in, pool_in, grads, arrived_rows,
    table, raw, lens, cot, ids, stage, ids_buf, cot_buf, counts, halves, part, part_in, scaled, total, landed,
    id_send, id_recv, cot_send, cot_recv, pass_send,
    part_send, part_recv, pool_send, pool_recv, row_send, row_recv,
):
    features, bag, each = ids.shape
    width, rows_dev = table.shape
    owners = n // features
    rows_out = rows_dev // reps
    levels = reps.bit_length() - 1
    pairs = n // 2
    me = lax.axis_index("dev")
    rep = lax.axis_index("rep")
    feature = me // owners
    lane = me % owners
    base = lane * rows_dev

    def flipped(value, bit):
        return value + (1 - 2 * (value // (1 << bit) % 2)) * (1 << bit)

    def near(step):
        return (me + step) % n

    def beside(step):
        return feature * owners + (lane + step) % owners

    def across(step):
        return (feature + step) % features * owners + lane

    barrier = pltpu.get_barrier_semaphore()
    for step in range(1, n):
        pl.semaphore_signal(
            barrier, inc=1, device_id={"dev": near(step)}, device_id_type=pl.DeviceIdType.MESH
        )
    for level in range(levels):
        pl.semaphore_signal(
            barrier, inc=1, device_id={"rep": flipped(rep, level)},
            device_id_type=pl.DeviceIdType.MESH,
        )
    staged = [
        pltpu.make_async_copy(src, dst, stage.at[at])
        for at, (src, dst) in enumerate(
            ((ids_in, raw), (lens_in, lens), (cot_in, cot), (table_in, table))
        )
    ]
    for copy in staged:
        copy.start()
    staged[0].wait()
    staged[1].wait()
    slot_index = lax.broadcasted_iota(I32, (bag, each), 0)
    for at in range(features):
        ids[at] = jnp.where(slot_index < lens[at : at + 1], raw[at], -(1 << 20))
    staged[2].wait()
    ids_buf[me] = ids[feature]
    cot_buf[me] = cot[feature]
    pl.semaphore_wait(barrier, n - 1 + levels)

    def remote(src, dst, send, recv, axis, to):
        return pltpu.make_async_remote_copy(
            src_ref=src, dst_ref=dst, send_sem=send, recv_sem=recv,
            device_id={axis: to}, device_id_type=pl.DeviceIdType.MESH,
        )

    def id_copy(peer, source):
        return remote(
            ids.at[peer // owners], ids_buf.at[source],
            id_send.at[peer], id_recv.at[source], "dev", peer,
        )

    def cot_copy(peer, source):
        return remote(
            cot.at[peer // owners], cot_buf.at[source],
            cot_send.at[peer], cot_recv.at[source], "dev", peer,
        )

    def pass_copy(source, step):
        return remote(
            cot_buf.at[source], cot_buf.at[source],
            pass_send.at[source // owners, step], cot_recv.at[source], "dev", beside(step),
        )

    def part_copy(source, slot):
        return remote(
            part.at[source], part_in.at[slot], part_send.at[source], part_recv.at[slot],
            "dev", feature * owners + source % owners,
        )

    def pool_copy(source, slot):
        return remote(
            part.at[source], pool_in.at[slot],
            pool_send.at[source // owners], pool_recv.at[slot], "dev", source,
        )

    for step in range(1, n):
        id_copy(near(step), me).start()
    for step in range(1, owners):
        cot_copy(beside(step), me).start()
    for step in range(1, features):
        cot_copy(across(step), me).start()

    staged[3].wait()

    def split_table(tile, _):
        at = pl.ds(pl.multiple_of(tile * ROW_TILE, ROW_TILE), ROW_TILE)
        high, low = split_bits(table[:, at])
        halves[:width, at] = high
        halves[width:, at] = low
        return 0

    lax.fori_loop(0, rows_dev // ROW_TILE, split_table, 0)

    def pass_on(step):
        source = across(features - step)
        cot_copy(source, source).wait_recv()
        for side in range(1, owners):
            pass_copy(source, side).start()

    def pair_columns(pair):
        return pl.ds(pl.multiple_of(pair * 2 * each, 2 * each), 2 * each)

    def count_pair(pair, _):
        columns = pair_columns(pair)
        blocks = []
        for half in range(2):
            step = pair * 2 + half
            source = (me - step + n) % n

            @pl.when(step > 0)
            def _():
                id_copy(source, source).wait_recv()

            blocks.append(ids_buf[source])
        slots = jnp.concatenate(blocks, axis=1) - base
        keys, times = [], []
        for j in range(bag):
            own = slots[j : j + 1]
            same = (slots == own).astype(I32)
            repeat = jnp.sum(same, axis=0, keepdims=True)
            keep = (own >= 0) & (own < rows_dev)
            if j:
                keep = keep & (jnp.sum(same[:j], axis=0, keepdims=True) == 0)
            keys.append(jnp.where(keep, own, -1))
            times.append(jnp.broadcast_to(repeat.astype(F32), (16, 2 * each)).astype(BF16))

        def count_tile(tile, _):
            start = pl.multiple_of(tile * ROW_TILE, ROW_TILE)
            wanted = []
            for j in range(bag):
                local = keys[j] - start
                local = jnp.where((local >= 0) & (local < ROW_TILE), local, -1)
                wanted.append(jnp.broadcast_to(local.astype(F32), (16, 2 * each)).astype(BF16))
            row = lax.broadcasted_iota(I32, (16, 2 * each), 0).astype(F32)
            for group in range(ROW_TILE // 16):
                here = (row + 16.0 * group).astype(BF16)
                found = jnp.zeros((16, 2 * each), BF16)
                for j in range(bag):
                    found = jnp.where(wanted[j] == here, times[j], found)
                counts[pl.ds(start + 16 * group, 16), columns] = found
            return 0

        lax.fori_loop(0, rows_dev // ROW_TILE, count_tile, 0)

        @pl.when((pair > 0) & (pair < features))
        def _():
            pass_on(pair)

        return 0

    lax.fori_loop(0, pairs, count_pair, 0)
    for step in range(pairs, features):
        pass_on(step)

    def pool_pair(pair, _):
        both = jnp.dot(halves[...], counts[:, pair_columns(pair)], preferred_element_type=F32)
        pool = both[:width] + both[width:]
        for half in range(2):
            source = (me - (pair * 2 + half) + n) % n
            part[source] = pool[:, half * each : (half + 1) * each]

            @pl.when(source % owners != lane)
            def _():
                part_copy(source, source // owners * owners + lane).start()

        return 0

    lax.fori_loop(0, pairs, pool_pair, 0)

    def scale_step(step, _):
        source = (me - step + n) % n

        @pl.when(source % owners != lane)
        def _():
            cot_copy(source, source).wait_recv()

        live = jnp.sum((ids_buf[source] >= 0).astype(F32), axis=0, keepdims=True)
        high, low = split_bits(cot_buf[source] * (1.0 / live))
        columns = pl.ds(pl.multiple_of(step * each, each), each)
        scaled[:width, columns] = high
        scaled[width:, columns] = low
        return 0

    lax.fori_loop(0, n, scale_step, 0)

    def grad_tile(chunk, tile):
        start = pl.multiple_of(chunk * rows_out + tile * ROW_TILE, ROW_TILE)
        both = lax.dot_general(
            scaled[...], counts[pl.ds(start, ROW_TILE), :], (((1,), (1,)), ((), ())),
            preferred_element_type=F32,
        )
        return both[:width] + both[width:]

    first = [0]
    for level in range(levels):
        first.append(first[-1] + (1 << (levels - 1 - level)))

    tiles = rows_out // ROW_TILE

    def row_copy(slot, level, tile):
        return remote(
            total.at[slot, tile], landed.at[slot, tile],
            row_send.at[slot, tile], row_recv.at[slot, tile],
            "rep", flipped(rep, level),
        )

    def sum_parts(step):
        source = across(step)
        value = part[source]
        for side in range(1, owners):
            slot = source // owners * owners + (lane + side) % owners
            part_copy(source, slot).wait_recv()
            value = value + part_in[slot]
        if step:
            part[source] = value
            pool_copy(source, feature).start()
        else:
            pool_in[feature] = value

    def place(apart):
        level, chunk = 0, rep
        while level < levels and not apart >> level & 1:
            level += 1
        for bit in range(levels):
            if apart >> bit & 1:
                chunk = flipped(chunk, bit)
        return level, chunk, first[level] + chunk // (1 << (level + 1)) if apart else 0

    def make_tile(apart, tile):
        level, chunk, slot = place(apart)
        value = grad_tile(chunk, tile)
        for before in range(level):
            if apart or before < levels - 1:
                came = first[before] + chunk // (1 << (before + 1))
                row_copy(came, before, tile).wait_recv()
                value = value + landed[came, tile]
        if apart:
            total[slot, tile] = value
            row_copy(slot, level, tile).start()
        else:
            grads[:, tile * ROW_TILE : (tile + 1) * ROW_TILE] = value

    far = reps // 2
    for tile in range(tiles + 1):
        for apart in reversed(range(far, reps)):
            late = 1 - apart % 2
            if 0 <= tile - late < tiles:
                make_tile(apart, tile - late)
    for apart in reversed(range(far)):
        if apart == 0:
            for step in reversed(range(features)):
                sum_parts(step)
        for tile in range(tiles):
            make_tile(apart, tile)
    for step in range(1, features):
        pool_copy(across(step), across(step) // owners).wait_recv()
    came = first[levels - 1] + rep // (1 << levels)
    for tile in range(tiles):
        row_copy(came, levels - 1, tile).wait_recv()
        arrived_rows[:, tile * ROW_TILE : (tile + 1) * ROW_TILE] = landed[came, tile]

    for apart in range(1, reps):
        level, _, slot = place(apart)
        for tile in range(tiles):
            row_copy(slot, level, tile).wait_send()
    for step in range(1, n):
        id_copy(near(step), me).wait_send()
    for step in range(1, owners):
        cot_copy(beside(step), me).wait_send()
    for step in range(1, features):
        source = across(step)
        cot_copy(source, me).wait_send()
        pool_copy(source, feature).wait_send()
        for side in range(1, owners):
            pass_copy(source, side).wait_send()
    for at in range(features):
        for side in range(1, owners):
            source = at * owners + (lane + side) % owners
            part_copy(source, at * owners + lane).wait_send()


def finish(lens, pool, own, arrived, pooled, grads):
    for at in range(pool.shape[0]):
        pooled[at] = pool[at] * (1.0 / lens[at : at + 1].astype(F32))
    grads[...] = own[...] + arrived[...]


def body(n, reps, emb_table, feature_ids, lengths, cotangent):
    rows_dev, width = emb_table.shape
    each, features, bag = feature_ids.shape
    lens = lengths.T
    rows_out = rows_dev // reps
    tiles = rows_out // ROW_TILE
    sem = pltpu.SemaphoreType.DMA
    vmem = pl.BlockSpec(memory_space=pltpu.VMEM)
    pool_shape = jax.ShapeDtypeStruct((features, width, each), F32)
    rows_shape = jax.ShapeDtypeStruct((width, rows_out), F32)
    pool, own, arrived = pl.pallas_call(
        functools.partial(kernel, n, reps),
        out_shape=(pool_shape, rows_shape, rows_shape),
        in_specs=[pl.BlockSpec(memory_space=pl.ANY)] * 4,
        out_specs=[vmem] * 3,
        scratch_shapes=[
            pltpu.VMEM((width, rows_dev), F32),
            pltpu.VMEM((features, bag, each), I32),
            pltpu.VMEM((features, each), I32),
            pltpu.VMEM((features, width, each), F32),
            pltpu.VMEM((features, bag, each), I32),
            sem((4,)),
            pltpu.VMEM((n, bag, each), I32),
            pltpu.VMEM((n, width, each), F32),
            pltpu.VMEM((rows_dev, n * each), BF16),
            pltpu.VMEM((2 * width, rows_dev), BF16),
            pltpu.VMEM((n, width, each), F32),
            pltpu.VMEM((n, width, each), F32),
            pltpu.VMEM((2 * width, n * each), BF16),
            pltpu.VMEM((reps - 1, tiles, width, ROW_TILE), F32),
            pltpu.VMEM((reps - 1, tiles, width, ROW_TILE), F32),
            sem((n,)), sem((n,)), sem((n,)), sem((n,)), sem((features, n // features)),
            sem((n,)), sem((n,)), sem((features,)), sem((features,)),
            sem((reps - 1, tiles)), sem((reps - 1, tiles)),
        ],
        compiler_params=pltpu.CompilerParams(
            collective_id=0, has_side_effects=True, vmem_limit_bytes=60 * 1024 * 1024
        ),
    )(
        emb_table.T, jnp.transpose(feature_ids, (1, 2, 0)), lens,
        jnp.transpose(cotangent, (1, 2, 0)),
    )
    pooled, grads = pl.pallas_call(
        finish,
        out_shape=(pool_shape, rows_shape),
        in_specs=[vmem] * 4,
        out_specs=[vmem] * 2,
    )(lens, pool, own, arrived)
    return jnp.transpose(pooled, (2, 0, 1)), grads.T


def solution(mesh):
    return jax.shard_map(
        functools.partial(body, mesh.shape["dev"], mesh.shape["rep"]),
        mesh=mesh,
        in_specs=(
            P("dev", None),
            P(("dev", "rep"), None, None),
            P(("dev", "rep"), None),
            P(("dev", "rep"), None, None),
        ),
        out_specs=(P(("dev", "rep"), None, None), P(("dev", "rep"), None)),
        check_vma=False,
    )
```
